128 devices in a mesh: dp: 64 (over x, y, z), mp: 2 (over core).
Axes of the slice: x: 4, y: 4, z: 4, core: 2. Of those that a mesh axis runs over, the one named last changes fastest.
Arguments:
- view_one: bfloat16 [32768, 1024], P('dp'), may hold values from -40 to 40
- view_two: bfloat16 [32768, 1024], P('dp'), may hold values from -40 to 40
Outputs:
- gradient_one: bfloat16 [32768, 1024], P(('dp', 'mp'))
- gradient_two: bfloat16 [32768, 1024], P(('dp', 'mp'))
- loss_value: float32 [], replicated
The draws below stay inside these ranges and needn't reach their ends.
All inputs are finite; a program needn't handle non-finite values.
Results may differ from the reference program's by a relative error of at most 0.013.
The reference program's roundings to bfloat16 on the way (of `coupling`, `normed_root` and `polar`) count: a program that leaves them out, or rounds other values in their place, can miss the bound.
Values may be sent and summed in bfloat16 or wider, within the bound.
A program may use at most 64 MiB of HBM per device.

```python
import math
import jax
import jax.numpy as jnp
from jax import lax

D = 1024
ITERS = 3
SQRT_ITERS = 2
N = 32768


def embedding_pair(key):
    trend_factor = 1.0 + 2.0 * jnp.arange(N, dtype=jnp.float32)[:, None] / N
    column_place = jnp.arange(D, dtype=jnp.float32)[None, :] / (D - 1)
    shared = jax.random.truncated_normal(jax.random.fold_in(key, 11), -4.0, 4.0, (N, D), jnp.float32)
    noise_one = jax.random.truncated_normal(jax.random.fold_in(key, 12), -4.0, 4.0, (N, D), jnp.float32)
    noise_two = jax.random.truncated_normal(jax.random.fold_in(key, 13), -4.0, 4.0, (N, D), jnp.float32)
    lowest = 0.3
    highest = 3.0
    share_low = 0.3
    share_high = 3.0
    share_weight = jnp.exp(math.log(share_low) + (math.log(share_high) - math.log(share_low)) * column_place)
    mixed_one = shared + 0.8 * noise_one
    mixed_two = share_weight * jnp.roll(shared, 11, axis=1) + 0.8 * noise_two
    mixed_one = mixed_one + 0.5 * jnp.roll(mixed_one, 1, axis=1) - 0.4 * jnp.roll(mixed_one, 37, axis=1)
    mixed_two = mixed_two + 0.5 * jnp.roll(mixed_two, 3, axis=1) - 0.4 * jnp.roll(mixed_two, 59, axis=1)
    scale_one = jnp.exp(jax.random.uniform(jax.random.fold_in(key, 15), (D,), jnp.float32, math.log(lowest), math.log(highest)))
    scale_two = jnp.exp(jax.random.uniform(jax.random.fold_in(key, 16), (D,), jnp.float32, math.log(lowest), math.log(highest)))
    offset_one = jax.random.normal(jax.random.fold_in(key, 17), (D,), jnp.float32)
    offset_two = jax.random.normal(jax.random.fold_in(key, 18), (D,), jnp.float32)
    view_one = jnp.clip(trend_factor * (offset_one + scale_one * mixed_one), -40.0, 40.0)
    view_two = jnp.clip(trend_factor * (offset_two + scale_two * mixed_two), -40.0, 40.0)
    return (view_one, view_two)


def draw_view_one(key, part):
    return embedding_pair(key)[0].astype(jnp.bfloat16)


def draw_view_two(key, part):
    return embedding_pair(key)[1].astype(jnp.bfloat16)


def setup_inputs(seed: int = 0) -> dict:
    streams_of = jax.random.split(jax.random.key(seed), 3)
    return {
        "view_one": draw_view_one(jax.random.fold_in(streams_of[2], 71), 0),
        "view_two": draw_view_two(jax.random.fold_in(streams_of[2], 71), 0),
    }


epsilon = 1e-06

def column_bound(matrix):
    return jnp.max(lax.optimization_barrier(jnp.sum(jnp.abs(matrix), axis=0))) + epsilon

def newton_schulz(normed, count):
    identity = jnp.eye(normed.shape[0], dtype=jnp.float32)
    iterate = identity.astype(jnp.bfloat16)
    final = identity
    for number in range(count):
        product = jnp.dot(iterate, normed, preferred_element_type=jnp.float32).astype(jnp.bfloat16)
        target = (1.5 * identity - 0.5 * jnp.dot(iterate, product, preferred_element_type=jnp.float32)).astype(jnp.bfloat16)
        final = jnp.dot(iterate, target, preferred_element_type=jnp.float32)
        iterate = final.astype(jnp.bfloat16)
    return final

def reference(view_one, view_two):
    mean_one = lax.optimization_barrier(jnp.sum(view_one, axis=0, dtype=jnp.float32)) / N
    mean_two = lax.optimization_barrier(jnp.sum(view_two, axis=0, dtype=jnp.float32)) / N
    gram_one = jnp.dot(view_one.T, view_one, preferred_element_type=jnp.float32)
    gram_two = jnp.dot(view_two.T, view_two, preferred_element_type=jnp.float32)
    gram_cross = jnp.dot(view_one.T, view_two, preferred_element_type=jnp.float32)
    cov_one = (gram_one - N * jnp.outer(mean_one, mean_one)) / (N - 1)
    cov_two = (gram_two - N * jnp.outer(mean_two, mean_two)) / (N - 1)
    cov_cross = (gram_cross - N * jnp.outer(mean_one, mean_two)) / (N - 1)
    bound_one = column_bound(cov_one)
    bound_two = column_bound(cov_two)
    normed_one = (cov_one / bound_one).astype(jnp.bfloat16)
    normed_two = (cov_two / bound_two).astype(jnp.bfloat16)
    cross = cov_cross.astype(jnp.bfloat16)
    final_one = newton_schulz(normed_one, ITERS)
    final_two = newton_schulz(normed_two, ITERS)
    white_one = (final_one / jnp.sqrt(bound_one)).astype(jnp.bfloat16)
    white_two = (final_two / jnp.sqrt(bound_two)).astype(jnp.bfloat16)
    inner = jnp.dot(cross, white_two, preferred_element_type=jnp.float32).astype(jnp.bfloat16)
    coupling = jnp.dot(white_one, inner, preferred_element_type=jnp.float32).astype(jnp.bfloat16)
    coupling_gram = jnp.dot(coupling.T, coupling, preferred_element_type=jnp.float32)
    bound_root = column_bound(coupling_gram)
    normed_root = (coupling_gram / bound_root).astype(jnp.bfloat16)
    final_root = newton_schulz(normed_root, SQRT_ITERS)
    loss_value = -jnp.sqrt(bound_root) * jnp.sum(normed_root.astype(jnp.float32) * final_root) / D
    root_inv = (final_root / jnp.sqrt(bound_root)).astype(jnp.bfloat16)
    polar = jnp.dot(coupling, root_inv, preferred_element_type=jnp.float32).astype(jnp.bfloat16)
    centered_one = (view_one.astype(jnp.float32) - mean_one).astype(jnp.bfloat16)
    centered_two = (view_two.astype(jnp.float32) - mean_two).astype(jnp.bfloat16)
    whitened_one = jnp.dot(centered_one, white_one, preferred_element_type=jnp.float32).astype(jnp.bfloat16)
    whitened_two = jnp.dot(centered_two, white_two, preferred_element_type=jnp.float32).astype(jnp.bfloat16)
    aligned_one = jnp.dot(whitened_one, polar, preferred_element_type=jnp.float32)
    aligned_two = jnp.dot(whitened_two, polar.T, preferred_element_type=jnp.float32)
    difference_one = (jnp.dot(aligned_one.astype(jnp.bfloat16), coupling.T, preferred_element_type=jnp.float32) - aligned_two).astype(jnp.bfloat16)
    difference_two = (jnp.dot(aligned_two.astype(jnp.bfloat16), coupling, preferred_element_type=jnp.float32) - aligned_one).astype(jnp.bfloat16)
    gradient_one = jnp.dot(difference_one, white_one, preferred_element_type=jnp.float32).astype(jnp.bfloat16)
    gradient_two = jnp.dot(difference_two, white_two, preferred_element_type=jnp.float32).astype(jnp.bfloat16)
    return (gradient_one, gradient_two, loss_value)
```

```python
import jax
import jax.numpy as jnp
from jax import lax
from jax.experimental import pallas as pl
from jax.experimental.pallas import tpu as pltpu
from jax.sharding import PartitionSpec as P

MESH = pl.DeviceIdType.MESH
F32, BF16 = jnp.float32, jnp.bfloat16
EPS = 1e-6
RING = 4
WIDTH = 1024
BLK = 256
NBLK = WIDTH // BLK
COLS = (((0,), (0,)), ((), ()))
ROWS = (((1,), (1,)), ((), ()))
JOBS = ((0, 2, 0), (128, 2, 1), (256, 1, 2), (320, 1, 0), (384, 1, 1), (448, 2, 2))
GRAM, CROSS = (0, 1, 2), (3, 4, 5)
AXES = ((0, 1, 2), (1, 2, 0), (2, 0, 1))
OFFSETS = (0, 32, 64, 80, 96, 112)


def dot(a, b):
    return jnp.dot(a, b, preferred_element_type=F32)


def kernel(
    total_rows, one_hbm, two_hbm, grad_one, grad_two, loss_ref,
    vs, pb, r1, r2, r3, sb, sr, mb, cb, xo, an, z, zn, w, xm, cm, ct, cg, pol, p_s, t_s,
    local_sem, send_sem, recv_sem, sum_send, sum_recv, w_send, w_recv, x_send, x_recv,
):
    dp, core = lax.axis_index("dp"), lax.axis_index("mp")
    at = (dp // 16, (dp // 4) % 4, dp % 4)
    rows = vs.shape[1]

    def peer(axis, k):
        place = list(at)
        place[axis] = (place[axis] + k) % RING
        return (place[0] * 16 + place[1] * 4 + place[2], core)

    partner = (dp, 1 - core)
    loads = [
        pltpu.make_async_copy(src, vs.at[i], local_sem.at[i])
        for i, src in enumerate((one_hbm, two_hbm))
    ]
    for load in loads:
        load.start()
    barrier = pltpu.get_barrier_semaphore()
    for axis in range(3):
        for k in range(1, RING):
            pl.semaphore_signal(barrier, inc=1, device_id=peer(axis, k), device_id_type=MESH)
    pl.semaphore_signal(barrier, inc=1, device_id=partner, device_id_type=MESH)
    for load in loads:
        load.wait()

    ones = jnp.ones((8, rows), BF16)
    for v in range(2):
        s = dot(ones, vs[v])
        for k in range(8):
            sb[0, v * 8 + k : v * 8 + k + 1, :] = s[0:1, 128 * k : 128 * k + 128]
    tile = 0
    for bi in range(NBLK):
        g = lax.dot_general(
            vs[core, :, BLK * bi : BLK * bi + BLK], vs[core, :, BLK * bi :], COLS,
            preferred_element_type=F32,
        )
        for h in range(g.shape[1] // 128):
            pb[tile : tile + 16] = g[:, 128 * h : 128 * h + 128].reshape(16, 16, 128)
            tile += 16
    for r in range(2):
        start = pl.multiple_of(core * 512 + r * BLK, BLK)
        g = lax.dot_general(
            vs[0, :, pl.ds(start, BLK)], vs[1], COLS, preferred_element_type=F32
        )
        for h in range(8):
            pb[tile : tile + 16] = g[:, 128 * h : 128 * h + 128].reshape(16, 16, 128)
            tile += 16

    pl.semaphore_wait(barrier, 10)
    sends = []

    bases = []
    for base, t, order in JOBS:
        b = [jnp.int32(base)]
        for p in range(3):
            b.append(b[-1] + at[AXES[order][p]] * (t * 4 ** (2 - p)))
        bases.append(b)
    slots = (r1, r2, r3)

    for p in range(3):
        started = []
        copies = []
        for k in (2, 1, 3):
            copy = pltpu.make_async_remote_copy(
                src_ref=sb.at[p], dst_ref=sr.at[p, k - 1],
                send_sem=sum_send.at[p, k - 1], recv_sem=sum_recv.at[p, k - 1],
                device_id=peer(p, k), device_id_type=MESH,
            )
            copy.start()
            copies.append(copy)
        for k in (2, 1, 3):
            for j, (base, t, order) in enumerate(JOBS):
                n = t * 4 ** (2 - p)
                axis = AXES[order][p]
                to = (at[axis] + k) % RING
                copy = pltpu.make_async_remote_copy(
                    src_ref=pb.at[pl.ds(bases[j][p] + to * n, n)],
                    dst_ref=slots[p].at[k - 1, pl.ds(OFFSETS[j] // 4**p, n)],
                    send_sem=send_sem.at[p, j, k - 1], recv_sem=recv_sem.at[p, j, k - 1],
                    device_id=peer(axis, k), device_id_type=MESH,
                )
                copy.start()
                started.append((j, copy))
        for copy in copies:
            copy.wait_recv()
        sb[p + 1] = sb[p] + sr[p, 0] + sr[p, 1] + sr[p, 2]
        for j, (base, t, order) in enumerate(JOBS):
            for i, copy in started:
                if i == j:
                    copy.wait_recv()
            n = t * 4 ** (2 - p)
            mine = pl.ds(bases[j][p + 1], n)
            got = slice(OFFSETS[j] // 4**p, OFFSETS[j] // 4**p + n)
            pb[mine] = pb[mine] + slots[p][0, got] + slots[p][1, got] + slots[p][2, got]
        sends += copies + [copy for _, copy in started]

    for i in range(16):
        mb[i] = jnp.broadcast_to(sb[3, i : i + 1, :] / total_rows, (8, 128))
    lane = lax.broadcasted_iota(jnp.int32, (8, 128), 1)
    sub = lax.broadcasted_iota(jnp.int32, (8, 128), 0)

    def center(j):
        base, t, order = JOBS[j]
        for q in range(t):
            tile = bases[j][3] + q
            if j in GRAM:
                hb = tile // 16
                blk = hb // 2
                ge4 = jnp.where(blk >= 4, 1, 0)
                ge7 = jnp.where(blk >= 7, 1, 0)
                ge9 = jnp.where(blk >= 9, 1, 0)
                bi = ge4 + ge7 + ge9
                bj = blk - 4 * ge4 - 3 * ge7 - 2 * ge9 + bi
                row = bi * BLK + (tile % 16) * 16
                column = bj * 2 + hb % 2
                row_view, column_view = core, core
            else:
                hb = (tile - 320) // 16
                row = core * 512 + (hb // 8) * BLK + (tile % 16) * 16
                column = hb % 8
                row_view, column_view = 0, 1
            across = mb[column_view * 8 + column]
            down = mb[row_view * 8 + row // 128]
            halves = []
            for h in range(2):
                at_row = lane == (row % 128) + h * 8 + sub
                col = jnp.sum(jnp.where(at_row, down, 0.0), axis=1, keepdims=True)
                raw = pb[tile, h * 8 : h * 8 + 8, :]
                halves.append((raw - total_rows * (col * across)) * (1.0 / (total_rows - 1)))
            cb[tile] = jnp.concatenate(halves, axis=0).astype(BF16)

    def gather_start(p, group):
        out = []
        for k in (2, 1, 3):
            for j in group:
                base, t, order = JOBS[j]
                part = cb.at[pl.ds(bases[j][p + 1], t * 4 ** (2 - p))]
                copy = pltpu.make_async_remote_copy(
                    src_ref=part, dst_ref=part,
                    send_sem=send_sem.at[3 + p, j, k - 1], recv_sem=recv_sem.at[3 + p, j, k - 1],
                    device_id=peer(AXES[order][p], k), device_id_type=MESH,
                )
                copy.start()
                out.append(copy)
        return out

    def gather_wait(copies):
        for copy in copies:
            copy.wait_recv()
        sends.extend(copies)

    for j in range(6):
        center(j)
    for p in (2, 1, 0):
        flight = gather_start(p, GRAM)
        if p == 0:
            cross_flight = gather_start(2, CROSS)
        gather_wait(flight)

    tile = 0
    for bi in range(NBLK):
        for bj in range(bi, NBLK):
            for h in range(2):
                part = cb[tile : tile + 16].reshape(BLK, 128)
                left = BLK * bj + 128 * h
                an[BLK * bi : BLK * bi + BLK, left : left + 128] = part
                if bi != bj:
                    an[left : left + 128, BLK * bi : BLK * bi + BLK] = part.T
                tile += 16

    def columns(j):
        return pl.ds(pl.multiple_of(j * BLK, BLK), BLK)

    def identity(j):
        r = lax.broadcasted_iota(jnp.int32, (WIDTH, BLK), 0)
        c = lax.broadcasted_iota(jnp.int32, (WIDTH, BLK), 1)
        return jnp.where(r == c + j * BLK, 1.5, 0.0)

    def peak(j, top):
        return jnp.maximum(top, jnp.max(jnp.sum(jnp.abs(an[:, columns(j)].astype(F32)), axis=0)))

    bound = lax.fori_loop(0, NBLK, peak, jnp.float32(0.0)) + EPS
    scale = 1.0 / bound
    white_scale = lax.rsqrt(bound)

    def norm(j, _):
        a = (an[:, columns(j)].astype(F32) * scale).astype(BF16)
        an[:, columns(j)] = a
        z[:, columns(j)] = (identity(j) - 0.5 * a.astype(F32)).astype(BF16)
        return 0

    lax.fori_loop(0, NBLK, norm, 0)
    gather_wait(cross_flight)
    cross_flight = gather_start(1, CROSS)

    def step(it, j):
        p_s[...] = dot(it[...], an[:, columns(j)]).astype(BF16)
        t_s[...] = (identity(j) - 0.5 * dot(it[...], p_s[...])).astype(BF16)
        return dot(it[...], t_s[...])

    def first(j, _):
        zn[:, columns(j)] = step(z, j).astype(BF16)
        return 0

    lax.fori_loop(0, NBLK, first, 0)
    gather_wait(cross_flight)
    cross_flight = gather_start(0, CROSS)

    def white_copy(j):
        part = w.at[core, :, columns(j)]
        return pltpu.make_async_remote_copy(
            src_ref=part, dst_ref=part, send_sem=w_send.at[j], recv_sem=w_recv.at[j],
            device_id=partner, device_id_type=MESH,
        )

    def second(j, _):
        w[core, :, columns(j)] = (step(zn, j) * white_scale).astype(BF16)
        white_copy(j).start()
        return 0

    lax.fori_loop(0, NBLK, second, 0)
    gather_wait(cross_flight)
    cross_copy = pltpu.make_async_remote_copy(
        src_ref=cb.at[pl.ds(320, 256)], dst_ref=xo, send_sem=x_send, recv_sem=x_recv,
        device_id=partner, device_id_type=MESH,
    )
    cross_copy.start()

    def place(src, first_tile, half):
        for r in range(2):
            for q in range(8):
                t0 = first_tile + (r * 8 + q) * 16
                xm[pl.ds(pl.multiple_of(half * 512 + r * BLK, BLK), BLK), 128 * q : 128 * q + 128] = (
                    src[t0 : t0 + 16].reshape(BLK, 128)
                )

    place(cb, 320, core)
    share = rows // 2
    mine = pl.ds(pl.multiple_of(core * share, share), share)
    centered = []
    for v in range(2):
        mean = jnp.concatenate([mb[v * 8 + k][0:1, :] for k in range(8)], axis=1)
        centered.append((vs[v, mine, :].astype(F32) - mean).astype(BF16))
    for j in range(NBLK):
        copy = white_copy(j)
        copy.wait_recv()
        sends.append(copy)
    whitened = [dot(centered[v], w[v]).astype(BF16) for v in range(2)]
    cross_copy.wait_recv()
    sends.append(cross_copy)
    place(xo, 0, 1 - core)

    def couple(j, _):
        p_s[...] = dot(xm[...], w[1, :, columns(j)]).astype(BF16)
        c = dot(w[0], p_s[...]).astype(BF16)
        cm[:, columns(j)] = c
        ct[columns(j), :] = c.T
        return 0

    lax.fori_loop(0, NBLK, couple, 0)

    def root_gram(j, top):
        g = dot(ct[...], cm[:, columns(j)])
        cg[:, columns(j)] = g
        return jnp.maximum(top, jnp.max(jnp.sum(jnp.abs(g), axis=0)))

    bound_root = lax.fori_loop(0, NBLK, root_gram, jnp.float32(0.0)) + EPS
    root_scale = 1.0 / bound_root
    inverse_scale = lax.rsqrt(bound_root)

    def root_norm(j, _):
        a = (cg[:, columns(j)] * root_scale).astype(BF16)
        an[:, columns(j)] = a
        z[:, columns(j)] = (identity(j) - 0.5 * a.astype(F32)).astype(BF16)
        return 0

    lax.fori_loop(0, NBLK, root_norm, 0)

    def root(j, trace):
        f = step(z, j)
        p_s[...] = (f * inverse_scale).astype(BF16)
        trace = trace + jnp.sum(an[:, columns(j)].astype(F32) * f)
        pol[:, columns(j)] = dot(cm[...], p_s[...]).astype(BF16)
        return trace

    trace = lax.fori_loop(0, NBLK, root, jnp.float32(0.0))
    loss_ref[...] = jnp.full(loss_ref.shape, -(bound_root * inverse_scale) * trace / WIDTH, F32)

    aligned_one = dot(whitened[0], pol[...])
    aligned_two = lax.dot_general(whitened[1], pol[...], ROWS, preferred_element_type=F32)
    difference_one = (dot(aligned_one.astype(BF16), ct[...]) - aligned_two).astype(BF16)
    difference_two = (dot(aligned_two.astype(BF16), cm[...]) - aligned_one).astype(BF16)
    grad_one[...] = dot(difference_one, w[0]).astype(BF16)
    grad_two[...] = dot(difference_two, w[1]).astype(BF16)
    for copy in sends:
        copy.wait_send()


def per_device(view_one, view_two):
    rows, width = view_one.shape
    total_rows = rows * lax.axis_size("dp")

    def body(*refs):
        kernel(total_rows, *refs)

    square = pltpu.VMEM((width, width), BF16)
    tall = pltpu.VMEM((width, BLK), BF16)
    dma = pltpu.SemaphoreType.DMA
    grad_one, grad_two, loss = pl.pallas_call(
        body,
        name="cca",
        out_shape=(
            jax.ShapeDtypeStruct((rows // 2, width), BF16),
            jax.ShapeDtypeStruct((rows // 2, width), BF16),
            jax.ShapeDtypeStruct((8, 128), F32),
        ),
        in_specs=[pl.BlockSpec(memory_space=pl.ANY)] * 2,
        out_specs=[pl.BlockSpec(memory_space=pltpu.VMEM)] * 3,
        scratch_shapes=[
            pltpu.VMEM((2, rows, width), BF16),
            pltpu.VMEM((576, 16, 128), F32),
            pltpu.VMEM((3, 144, 16, 128), F32),
            pltpu.VMEM((3, 36, 16, 128), F32),
            pltpu.VMEM((3, 9, 16, 128), F32),
            pltpu.VMEM((4, 16, 128), F32),
            pltpu.VMEM((3, 3, 16, 128), F32),
            pltpu.VMEM((16, 8, 128), F32),
            pltpu.VMEM((576, 16, 128), BF16),
            pltpu.VMEM((256, 16, 128), BF16),
            square, square, square,
            pltpu.VMEM((2, width, width), BF16),
            square, square, square,
            pltpu.VMEM((width, width), F32),
            square, tall, tall,
            dma((2,)), dma((6, 6, 3)), dma((6, 6, 3)), dma((3, 3)), dma((3, 3)),
            dma((4,)), dma((4,)), dma, dma,
        ],
        compiler_params=pltpu.CompilerParams(
            collective_id=0, has_side_effects=True, vmem_limit_bytes=62 << 20
        ),
    )(view_one, view_two)
    return grad_one, grad_two, loss[0, 0]


def solution(mesh):
    return jax.shard_map(
        per_device,
        mesh=mesh,
        in_specs=(P("dp", None), P("dp", None)),
        out_specs=(P(("dp", "mp"), None), P(("dp", "mp"), None), P()),
        check_vma=False,
    )
```
